32 devices in a mesh: sp: 32 (over z, y, x, core).
Axes of the slice: x: 2, y: 2, z: 4, core: 2. Of those that a mesh axis runs over, the one named last changes fastest.
Arguments:
- x: bfloat16 [4, 4096, 2048], P(None, 'sp')
- d_y: bfloat16 [4, 4096, 2048], P(None, 'sp')
- ln_gamma: bfloat16 [2048], replicated
- ln_beta: bfloat16 [2048], replicated
- w_qkv: bfloat16 [2048, 6144], replicated
- b_qkv: bfloat16 [6144], replicated
- w_out: bfloat16 [2048, 2048], replicated
- b_out: bfloat16 [2048], replicated
- head_kind: int32 [32], replicated
Outputs:
- output 1: bfloat16 [4, 4096, 2048], P(None, 'sp')
- output 2: bfloat16 [4, 4096, 2048], P(None, 'sp')
- output 3: float32 [2048], replicated
- output 4: float32 [2048], replicated
- output 5: float32 [2048, 6144], replicated
- output 6: float32 [6144], replicated
- output 7: float32 [2048, 2048], replicated
- output 8: float32 [2048], replicated
All inputs are finite; a program needn't handle non-finite values.
Results may differ from the reference program's by a relative error of at most 0.0126655.
Values are sent between devices in bfloat16 or wider.
A program may use at most 1 GiB of HBM per device.

```python
import math
import jax
import jax.numpy as jnp
from jax import lax

BATCH_SIZE = 4
SEQ_LEN = 4096
D_MODEL = 2048
NUM_HEADS = 32
HEAD_DIM = D_MODEL // NUM_HEADS
BAND_WIDTH = SEQ_LEN // 4
QUERY_BLOCK = min(128, SEQ_LEN)
SCORE_SCALE = 1.0 / math.sqrt(HEAD_DIM)
LN_EPS = 1e-5
NEG_BIG = -1e30


def setup_inputs(seed: int = 0) -> dict:
    key_list = jax.random.split(jax.random.key(seed), 9)
    tok_shape = (BATCH_SIZE, SEQ_LEN, D_MODEL)
    w_scale = 1.0 / math.sqrt(D_MODEL)
    qkv_gain = jnp.array([1.7, 1.7, 1.0], jnp.float32)
    x_val = jax.random.normal(key_list[0], tok_shape, jnp.float32)
    dy_val = jax.random.normal(key_list[1], tok_shape, jnp.float32)
    gamma_val = 1.0 + 0.3 * jax.random.normal(key_list[2], (D_MODEL,), jnp.float32)
    beta_val = 0.3 * jax.random.normal(key_list[3], (D_MODEL,), jnp.float32)
    wqkv_val = jax.random.normal(key_list[4], (D_MODEL, 3, D_MODEL), jnp.float32) * qkv_gain[None, :, None] * w_scale
    bqkv_val = 0.5 * jax.random.normal(key_list[5], (3 * D_MODEL,), jnp.float32)
    wout_val = jax.random.normal(key_list[6], (D_MODEL, D_MODEL), jnp.float32) * w_scale
    bout_val = 0.5 * jax.random.normal(key_list[7], (D_MODEL,), jnp.float32)
    kind_val = (jax.random.permutation(key_list[8], NUM_HEADS) < NUM_HEADS // 2).astype(jnp.int32)
    return {
        "x": x_val.astype(jnp.bfloat16),
        "d_y": dy_val.astype(jnp.bfloat16),
        "ln_gamma": gamma_val.astype(jnp.bfloat16),
        "ln_beta": beta_val.astype(jnp.bfloat16),
        "w_qkv": wqkv_val.reshape(D_MODEL, 3 * D_MODEL).astype(jnp.bfloat16),
        "b_qkv": bqkv_val.astype(jnp.bfloat16),
        "w_out": wout_val.astype(jnp.bfloat16),
        "b_out": bout_val.astype(jnp.bfloat16),
        "head_kind": kind_val,
    }


def bf16_cast(values):
    return values.astype(jnp.bfloat16).astype(jnp.float32)


def layer_norm(x_rows, gamma_f, beta_f):
    row_mean = jnp.mean(x_rows, axis=-1, keepdims=True)
    centred = x_rows - row_mean
    row_var = jnp.mean(centred * centred, axis=-1, keepdims=True)
    return centred * lax.rsqrt(row_var + LN_EPS) * gamma_f + beta_f


def head_attention(q_head, k_head, v_head, banded):
    key_pos = jnp.arange(SEQ_LEN)[None, :]

    def query_block(q_start):
        q_part = lax.dynamic_slice_in_dim(q_head, q_start, QUERY_BLOCK, axis=1)
        logits = jnp.einsum("bqd,bkd->bqk", q_part, k_head) * SCORE_SCALE
        query_pos = q_start + jnp.arange(QUERY_BLOCK)[:, None]
        allowed = (key_pos <= query_pos) & ((banded == 0) | (key_pos > query_pos - BAND_WIDTH))
        attn_prob = jax.nn.softmax(jnp.where(allowed[None], logits, NEG_BIG), axis=-1)
        return bf16_cast(jnp.einsum("bqk,bkd->bqd", bf16_cast(attn_prob), v_head))

    return lax.map(jax.checkpoint(query_block), jnp.arange(SEQ_LEN // QUERY_BLOCK) * QUERY_BLOCK)


def block_forward(x_f, gamma_f, beta_f, wqkv_f, bqkv_f, wout_f, bout_f, head_kind):
    h_norm = bf16_cast(layer_norm(x_f, gamma_f, beta_f))
    qkv_tok = bf16_cast(jnp.dot(h_norm, wqkv_f, preferred_element_type=jnp.float32) + bqkv_f)
    qkv_head = jnp.transpose(qkv_tok.reshape(BATCH_SIZE, SEQ_LEN, 3, NUM_HEADS, HEAD_DIM), (2, 3, 0, 1, 4))

    def one_head(head_items):
        return head_attention(head_items[0], head_items[1], head_items[2], head_items[3])

    attn_heads = lax.map(one_head, (qkv_head[0], qkv_head[1], qkv_head[2], head_kind))
    attn_tok = jnp.transpose(attn_heads, (2, 1, 3, 0, 4)).reshape(BATCH_SIZE, SEQ_LEN, D_MODEL)
    return x_f + jnp.dot(attn_tok, wout_f, preferred_element_type=jnp.float32) + bout_f


def reference(x, d_y, ln_gamma, ln_beta, w_qkv, b_qkv, w_out, b_out, head_kind):
    def block_fn(x_f, gamma_f, beta_f, wqkv_f, bqkv_f, wout_f, bout_f):
        return block_forward(x_f, gamma_f, beta_f, wqkv_f, bqkv_f, wout_f, bout_f, head_kind)

    primal_list = [item_arr.astype(jnp.float32) for item_arr in (x, ln_gamma, ln_beta, w_qkv, b_qkv, w_out, b_out)]
    y_full, pull_back = jax.vjp(block_fn, *primal_list)
    grad_list = pull_back(d_y.astype(jnp.float32))
    return (y_full.astype(jnp.bfloat16), grad_list[0].astype(jnp.bfloat16), grad_list[1], grad_list[2], grad_list[3], grad_list[4], grad_list[5], grad_list[6])
```

```python
import math
import jax
import jax.numpy as jnp
from jax import lax
from jax.experimental import pallas as pl
from jax.experimental.pallas import tpu as pltpu
from jax.sharding import PartitionSpec as P

LN_EPS = 1e-5
NEG_BIG = -1e30
F32 = jnp.float32
BF16 = jnp.bfloat16
NT = (((1,), (1,)), ((), ()))
NN = (((1,), (0,)), ((), ()))
TILE = 128
WIDTH = 2048
DIM = 64
DEVS = 32
ROWS = 512
BAND = 1024
SEQ = 4096
BQ = 256
BK = 512
LOG2E = 1.4426950408889634


def dot(a, b, dims=NN):
    return lax.dot_general(a, b, dims, preferred_element_type=F32)


def params():
    return pltpu.CompilerParams(vmem_limit_bytes=56 * 2**20)


def low_lanes(shape):
    return lax.broadcasted_iota(jnp.int32, shape, len(shape) - 1) < DIM


def layer_norm(x_rows, gamma_f, beta_f):
    row_mean = jnp.mean(x_rows, axis=-1, keepdims=True)
    centred = x_rows - row_mean
    row_var = jnp.mean(centred * centred, axis=-1, keepdims=True)
    return centred * lax.rsqrt(row_var + LN_EPS) * gamma_f + beta_f


def project_kernel(kind_ref, k_ref, x_ref, w_ref, b_ref, out_ref, buf, sem, *, dims, steps):
    step = pl.program_id(0)
    side = lax.rem(step, 2)

    def copies(at):
        slot = lax.rem(at, 2)
        for i in range(8):
            n = lax.rem(at, 4) * 8 + i
            for half in range(2):
                yield pltpu.make_async_copy(
                    buf.at[slot, i, half],
                    out_ref.at[kind_ref[n], 2 * k_ref[n] + half, lax.div(at, 4)],
                    sem.at[slot],
                )

    @pl.when(step >= 2)
    def _():
        for copy in copies(step - 2):
            copy.wait()

    low = low_lanes((TILE, TILE))
    for pair in range(4):
        cols = slice(pair * TILE, pair * TILE + TILE)
        w_part = w_ref[:, cols] if dims == NN else w_ref[cols, :]
        acc = dot(x_ref[...], w_part, dims) + b_ref[:, cols]
        for half in range(2):
            r0 = acc[half * 256 : half * 256 + TILE]
            r1 = acc[half * 256 + TILE : half * 256 + 256]
            buf[side, 2 * pair, half] = jnp.where(low, r0, pltpu.roll(r1, DIM, 1)).astype(BF16)
            buf[side, 2 * pair + 1, half] = jnp.where(low, pltpu.roll(r0, DIM, 1), r1).astype(BF16)
    for copy in copies(step):
        copy.start()

    @pl.when(step == steps - 1)
    def _():
        for copy in copies(step - 1):
            copy.wait()
        for copy in copies(step):
            copy.wait()


def project(x, w, bias, head_kind, head_k, transposed):
    cols = w.shape[0] if transposed else w.shape[1]
    steps = cols // ROWS
    if transposed:
        w_spec = pl.BlockSpec((ROWS, WIDTH), lambda c, *_: (c, 0))
    else:
        w_spec = pl.BlockSpec((WIDTH, ROWS), lambda c, *_: (0, c))
    body = lambda *refs: project_kernel(*refs, dims=NT if transposed else NN, steps=steps)
    return pl.pallas_call(
        body,
        out_shape=jax.ShapeDtypeStruct((2, DEVS, steps // 4, TILE, TILE), BF16),
        grid_spec=pltpu.PrefetchScalarGridSpec(
            num_scalar_prefetch=2,
            grid=(steps,),
            in_specs=[
                pl.BlockSpec((ROWS, WIDTH), lambda c, *_: (0, 0)),
                w_spec,
                pl.BlockSpec((1, ROWS), lambda c, *_: (0, c)),
            ],
            out_specs=pl.BlockSpec(memory_space=pl.ANY),
            scratch_shapes=[pltpu.VMEM((2, 8, 2, TILE, TILE), BF16), pltpu.SemaphoreType.DMA((2,))],
        ),
        compiler_params=params(),
        cost_estimate=pl.CostEstimate(flops=2 * ROWS * WIDTH * cols, bytes_accessed=WIDTH * cols * 2, transcendentals=0),
        name="project",
    )(head_kind, head_k, x, w, bias)


def unpack_kernel(kind_ref, k_ref, *refs):
    out_ref = refs[8]
    low = low_lanes((TILE, TILE))
    for pair in range(4):
        for half in range(2):
            a = refs[2 * pair][half].astype(F32)
            b = refs[2 * pair + 1][half].astype(F32)
            cols = slice(pair * TILE, pair * TILE + TILE)
            out_ref[half * 256 : half * 256 + TILE, cols] = jnp.where(low, a, pltpu.roll(b, DIM, 1)).astype(BF16)
            out_ref[half * 256 + TILE : half * 256 + 256, cols] = jnp.where(low, pltpu.roll(a, DIM, 1), b).astype(BF16)


def unpack(slots, head_kind, head_k):
    reps = slots.shape[2]
    slots = slots.reshape(2, 16, 2, reps, TILE, TILE)

    def spec(i):
        def index(c, kind_ref, k_ref):
            n = lax.rem(c, 4) * 8 + i
            return kind_ref[n], k_ref[n], 0, lax.div(c, 4), 0, 0

        return pl.BlockSpec((None, None, 2, None, TILE, TILE), index)

    return pl.pallas_call(
        unpack_kernel,
        out_shape=jax.ShapeDtypeStruct((ROWS, reps * WIDTH), BF16),
        grid_spec=pltpu.PrefetchScalarGridSpec(
            num_scalar_prefetch=2,
            grid=(4 * reps,),
            in_specs=[spec(i) for i in range(8)],
            out_specs=pl.BlockSpec((ROWS, ROWS), lambda c, *_: (0, c)),
        ),
        compiler_params=params(),
        cost_estimate=pl.CostEstimate(flops=reps * 2 * 10**9, bytes_accessed=reps * 2**22, transcendentals=0),
        name="unpack",
    )(head_kind, head_k, *([slots] * 8))


def unpack_weights_kernel(kind_ref, k_ref, *refs):
    out_ref = refs[8]
    group = pl.program_id(2)
    low = low_lanes((TILE, TILE))
    for pair in range(4):
        keep_a = kind_ref[group * 8 + 2 * pair] == 0
        keep_b = kind_ref[group * 8 + 2 * pair + 1] == 1

        def rows_step(r, carry, pair=pair, keep_a=keep_a, keep_b=keep_b):
            rows = pl.ds(pl.multiple_of(r * TILE, TILE), TILE)
            a = refs[2 * pair][rows].astype(F32)
            b = refs[2 * pair + 1][rows].astype(F32)
            a = jnp.where(keep_a, a, pltpu.roll(a, DIM, 1))
            b = jnp.where(keep_b, b, pltpu.roll(b, DIM, 1))
            out_ref[rows, pair * TILE : pair * TILE + TILE] = jnp.where(low, a, b)
            return carry

        lax.fori_loop(0, 4, rows_step, 0)


def unpack_weights(gathered, head_kind, head_k):
    def spec(i):
        def index(rh, t, g, kind_ref, k_ref):
            k = k_ref[g * 8 + i]
            fx = lax.div(rh, 2)
            other = lax.rem(k + fx, 2)
            return lax.div(k, 2) * 2 + fx, lax.rem(rh, 2), other * 3 + t, 0, 0

        return pl.BlockSpec((None, None, None, ROWS, TILE), index)

    return pl.pallas_call(
        unpack_weights_kernel,
        out_shape=jax.ShapeDtypeStruct((WIDTH, 3 * WIDTH), F32),
        grid_spec=pltpu.PrefetchScalarGridSpec(
            num_scalar_prefetch=2,
            grid=(4, 3, 4),
            in_specs=[spec(i) for i in range(8)],
            out_specs=pl.BlockSpec((ROWS, ROWS), lambda rh, t, g, *_: (rh, t * 4 + g)),
        ),
        compiler_params=params(),
        cost_estimate=pl.CostEstimate(flops=20 * 10**9, bytes_accessed=100 * 2**20, transcendentals=0),
        name="unpack_weights",
    )(head_kind, head_k, *([gathered] * 8))


def unpack_out(gathered):
    def index(rh, c):
        k = lax.rem(c, 2) * 8 + lax.rem(lax.div(c, 2), 2) * 4 + lax.rem(lax.div(c, 4), 2) * 2 + lax.div(c, 8)
        return k, rh, 3, 0, 0

    def body(in_ref, out_ref):
        out_ref[...] = in_ref[...].reshape(BAND, TILE).astype(F32)

    return pl.pallas_call(
        body,
        out_shape=jax.ShapeDtypeStruct((WIDTH, WIDTH), F32),
        grid=(2, 16),
        in_specs=[pl.BlockSpec((None, None, 2, ROWS, TILE), index)],
        out_specs=pl.BlockSpec((BAND, TILE), lambda rh, c: (rh, c)),
        compiler_params=params(),
        cost_estimate=pl.CostEstimate(flops=5 * 10**9, bytes_accessed=24 * 2**20, transcendentals=0),
        name="unpack_out",
    )(gathered)


def regroup_kernel(f_ref, b_ref, out_ref):
    low = low_lanes((TILE, TILE))
    for r in range(4):
        for t in range(3):
            f = f_ref[r, t].astype(F32)
            b = b_ref[r, t].astype(F32)
            rows = slice(t * TILE, t * TILE + TILE)
            even = jnp.where(low, f, pltpu.roll(b, DIM, 1))
            odd = jnp.where(low, pltpu.roll(f, DIM, 1), b)
            out_ref[rows, r * 256 : r * 256 + TILE] = jnp.transpose(even).astype(BF16)
            out_ref[rows, r * 256 + TILE : r * 256 + 256] = jnp.transpose(odd).astype(BF16)


def regroup(f_slots, b_slots):
    spec = pl.BlockSpec((4, 3, TILE, TILE), lambda r: (r, 0, 0, 0))
    return pl.pallas_call(
        regroup_kernel,
        out_shape=jax.ShapeDtypeStruct((384, 8192), BF16),
        grid=(8,),
        in_specs=[spec, spec],
        out_specs=pl.BlockSpec((384, BAND), lambda r: (0, r)),
        compiler_params=params(),
        cost_estimate=pl.CostEstimate(flops=5 * 10**9, bytes_accessed=12 * 2**20, transcendentals=0),
        name="regroup",
    )(f_slots, b_slots)


def split_pair(rows):
    low = low_lanes(rows.shape)
    zero = jnp.zeros_like(rows)
    return jnp.concatenate([jnp.where(low, rows, zero), jnp.where(low, zero, rows)], axis=0)


def load_rows(ref, index, blocks):
    return ref[pl.ds(index * blocks, blocks)].reshape(blocks * TILE, TILE)


def transpose_into(src_ref, dst):
    def step(r, carry):
        cols = pl.ds(pl.multiple_of(r * TILE, TILE), TILE)
        dst[:, cols] = jnp.transpose(src_ref[r].astype(F32)).astype(BF16)
        return carry

    lax.fori_loop(0, DEVS, step, 0)


def allowed_mask(i, j, banded):
    shape = (BK, 2 * BQ)
    diff = lax.broadcasted_iota(jnp.int32, shape, 0) - (lax.broadcasted_iota(jnp.int32, shape, 1) & (BQ - 1))
    off = i * BQ - j * BK
    keep = diff <= off
    if banded:
        keep = keep & (diff > off - BAND)
    return keep


def forward_kernel(q_ref, k_ref, v_ref, o_ref, lse_ref, v_t, *, banded, scale2):
    transpose_into(v_ref, v_t)

    def q_block(i, carry):
        q_pair = split_pair(load_rows(q_ref, i, 2))

        def scores(j, masked):
            s_t = dot(load_rows(k_ref, j, 4), q_pair, NT)
            return jnp.where(allowed_mask(i, j, banded), s_t, NEG_BIG) if masked else s_t

        def weighted(j, p_t):
            cols = pl.ds(pl.multiple_of(j * BK, BK), BK)
            p_t = p_t.astype(BF16)
            return jnp.concatenate(
                [dot(v_t[0:DIM, cols], p_t[:, 0:BQ]), dot(v_t[DIM:TILE, cols], p_t[:, BQ : 2 * BQ])], axis=1
            )

        last = lax.div(i, 2)
        s_t = scores(last, True)
        m = jnp.max(s_t, axis=0, keepdims=True)
        p_t = jnp.exp2((s_t - m) * scale2)
        state = m, jnp.sum(p_t, axis=0, keepdims=True), weighted(last, p_t)

        def k_block(j, state, masked):
            m, l, acc = state
            s_t = scores(j, masked)
            m_new = jnp.maximum(m, jnp.max(s_t, axis=0, keepdims=True))
            p_t = jnp.exp2((s_t - m_new) * scale2)
            fade = jnp.exp2((m - m_new) * scale2)
            return m_new, l * fade + jnp.sum(p_t, axis=0, keepdims=True), acc * fade + weighted(j, p_t)

        if banded:
            near = jnp.maximum(last - 1, 0)
            state = lax.fori_loop(near, last, lambda j, c: k_block(j, c, False), state)
            state = lax.fori_loop(jnp.maximum(last - 2, 0), near, lambda j, c: k_block(j, c, True), state)
        else:
            state = lax.fori_loop(0, last, lambda j, c: k_block(j, c, False), state)
        m, l, acc = state
        out = acc / l
        out = jnp.transpose(jnp.concatenate([out[:, 0:BQ], out[:, BQ : 2 * BQ]], axis=0))
        o_ref[pl.ds(i * 2, 2)] = out.astype(BF16).reshape(2, TILE, TILE)
        lse_ref[pl.ds(i, 1), :] = m * scale2 + jnp.log2(l)
        return carry

    lax.fori_loop(0, SEQ // BQ, q_block, 0)


def attend_forward(qkv, banded):
    scale2 = LOG2E / math.sqrt(DIM)
    whole = lambda t: pl.BlockSpec((DEVS, None, TILE, TILE), lambda g: (0, t, 0, 0))
    tiles = 42 if banded else 72
    return pl.pallas_call(
        lambda *refs: forward_kernel(*refs, banded=banded, scale2=scale2),
        out_shape=(jax.ShapeDtypeStruct((DEVS, TILE, TILE), BF16), jax.ShapeDtypeStruct((16, 2 * BQ), F32)),
        grid=(1,),
        in_specs=[whole(0), whole(1), whole(2)],
        out_specs=(
            pl.BlockSpec((DEVS, TILE, TILE), lambda g: (0, 0, 0)),
            pl.BlockSpec((16, 2 * BQ), lambda g: (0, 0)),
        ),
        scratch_shapes=[pltpu.VMEM((TILE, SEQ), BF16)],
        compiler_params=params(),
        cost_estimate=pl.CostEstimate(flops=tiles * 5 * 10**8, bytes_accessed=2**22, transcendentals=tiles * 2**18),
        name="forward_band" if banded else "forward_full",
    )(qkv, qkv, qkv)


def backward_kernel(q_ref, k_ref, v_ref, do_ref, o_ref, lse_ref, out_ref, k_t, dq_t, delta, dk_acc, dv_acc, *, banded, scale, scale2):
    transpose_into(k_ref, k_t)

    def prepare(i, carry):
        prod = jnp.transpose(load_rows(do_ref, i, 2).astype(F32) * load_rows(o_ref, i, 2).astype(F32))
        delta[pl.ds(i, 1), :] = jnp.concatenate(
            [jnp.sum(prod[0:DIM], axis=0, keepdims=True), jnp.sum(prod[DIM:TILE], axis=0, keepdims=True)], axis=1
        )
        dq_t[i] = jnp.zeros((TILE, BQ), F32)
        return carry

    lax.fori_loop(0, SEQ // BQ, prepare, 0)

    def k_block(j, carry):
        k_rows = load_rows(k_ref, j, 4)
        v_rows = load_rows(v_ref, j, 4)
        cols = pl.ds(pl.multiple_of(j * BK, BK), BK)
        dk_acc[...] = jnp.zeros_like(dk_acc)
        dv_acc[...] = jnp.zeros_like(dv_acc)

        def q_block(i, carry, masked):
            q_pair = split_pair(load_rows(q_ref, i, 2))
            do_pair = split_pair(load_rows(do_ref, i, 2))
            p_t = jnp.exp2(dot(k_rows, q_pair, NT) * scale2 - lse_ref[pl.ds(i, 1), :])
            if masked:
                p_t = jnp.where(allowed_mask(i, j, banded), p_t, 0.0)
            dp_t = dot(v_rows, do_pair, NT).astype(BF16).astype(F32)
            ds_t = (p_t * (dp_t - delta[pl.ds(i, 1), :]) * scale).astype(BF16)
            dv_acc[...] += dot(p_t.astype(BF16), do_pair)
            dk_acc[...] += dot(ds_t, q_pair)
            dq_t[i, 0:DIM, :] += dot(k_t[0:DIM, cols], ds_t[:, 0:BQ])
            dq_t[i, DIM:TILE, :] += dot(k_t[DIM:TILE, cols], ds_t[:, BQ : 2 * BQ])
            return carry

        first = 2 * j
        lax.fori_loop(first, first + 2, lambda i, c: q_block(i, c, True), 0)
        if banded:
            edge = jnp.minimum(first + 4, 16)
            lax.fori_loop(first + 2, edge, lambda i, c: q_block(i, c, False), 0)
            lax.fori_loop(edge, jnp.minimum(first + 6, 16), lambda i, c: q_block(i, c, True), 0)
        else:
            lax.fori_loop(first + 2, 16, lambda i, c: q_block(i, c, False), 0)
        out_ref[pl.ds(j * 4, 4), 1] = dk_acc[...].astype(BF16).reshape(4, TILE, TILE)
        out_ref[pl.ds(j * 4, 4), 2] = dv_acc[...].astype(BF16).reshape(4, TILE, TILE)
        return carry

    lax.fori_loop(0, SEQ // BK, k_block, 0)

    def finish(i, carry):
        out_ref[pl.ds(i * 2, 2), 0] = jnp.transpose(dq_t[i]).astype(BF16).reshape(2, TILE, TILE)
        return carry

    lax.fori_loop(0, SEQ // BQ, finish, 0)


def attend_backward(qkv, d_out, out, lse, banded):
    scale = 1.0 / math.sqrt(DIM)
    whole = lambda t: pl.BlockSpec((DEVS, None, TILE, TILE), lambda g: (0, t, 0, 0))
    flat = pl.BlockSpec((DEVS, TILE, TILE), lambda g: (0, 0, 0))
    of_kind = pl.BlockSpec((None, DEVS, TILE, TILE), lambda g: (1 if banded else 0, 0, 0, 0))
    tiles = 42 if banded else 72
    return pl.pallas_call(
        lambda *refs: backward_kernel(*refs, banded=banded, scale=scale, scale2=scale * LOG2E),
        out_shape=jax.ShapeDtypeStruct((DEVS, 3, TILE, TILE), BF16),
        grid=(1,),
        in_specs=[whole(0), whole(1), whole(2), of_kind, flat, pl.BlockSpec((16, 2 * BQ), lambda g: (0, 0))],
        out_specs=pl.BlockSpec((DEVS, 3, TILE, TILE), lambda g: (0, 0, 0, 0)),
        scratch_shapes=[
            pltpu.VMEM((TILE, SEQ), BF16),
            pltpu.VMEM((16, TILE, BQ), F32),
            pltpu.VMEM((16, 2 * BQ), F32),
            pltpu.VMEM((BK, TILE), F32),
            pltpu.VMEM((BK, TILE), F32),
        ],
        compiler_params=params(),
        cost_estimate=pl.CostEstimate(flops=tiles * 10**9, bytes_accessed=2**23, transcendentals=tiles * 2**18),
        name="backward_band" if banded else "backward_full",
    )(qkv, qkv, qkv, d_out, out, lse)


def exchange(slots):
    return lax.all_to_all(slots, "sp", 0, 0, tiled=True)


def solution(mesh):
    tok_spec = P(None, "sp", None)
    pair_swap = [(i, i ^ 1) for i in range(DEVS)]
    x_swap = [(i, i ^ 2) for i in range(DEVS)]
    same_xc = [list(range(c, DEVS, 4)) for c in range(4)]

    def layer(x, d_y, ln_gamma, ln_beta, w_qkv, b_qkv, w_out, b_out, head_kind):
        half = lax.rem(lax.axis_index("sp"), 2)
        x_bit = lax.rem(lax.div(lax.axis_index("sp"), 2), 2)
        head = jnp.arange(DEVS)
        banded_before = jnp.sum(jnp.where(head[None, :] < head[:, None], head_kind[None, :], 0), axis=1)
        head_k = jnp.where(head_kind == 1, banded_before, head - banded_before).astype(jnp.int32)

        x_f = x.astype(F32)
        h_f, ln_pull = jax.vjp(layer_norm, x_f, ln_gamma.astype(F32), ln_beta.astype(F32))
        h_norm = h_f.astype(BF16)
        d_y_rows = d_y.reshape(ROWS, WIDTH)

        def trade(array, bit, width, axis, flip):
            keep = lax.dynamic_slice_in_dim(array, bit * width, width, axis)
            take = lax.ppermute(lax.dynamic_slice_in_dim(array, width - bit * width, width, axis), "sp", flip)
            return jnp.where(bit == 0, jnp.stack([keep, take]), jnp.stack([take, keep]))

        h_part = trade(h_norm, half, 2, 0, pair_swap)
        h_part = trade(h_part, x_bit, BAND, 3, x_swap)
        h_all = lax.all_gather(h_part, "sp", axis_index_groups=same_xc).reshape(2 * SEQ, BAND)
        qkv_slots = project(h_norm.reshape(ROWS, WIDTH), w_qkv, b_qkv.astype(F32).reshape(1, 3 * WIDTH), head_kind, head_k, False)
        d_attn_slots = project(d_y_rows, w_out, jnp.zeros((1, WIDTH), F32), head_kind, head_k, True)
        qkv_full = exchange(qkv_slots[0])
        qkv_band = exchange(qkv_slots[1])
        qkv_full, d_attn_slots = lax.optimization_barrier((qkv_full, d_attn_slots))
        d_attn = lax.all_to_all(d_attn_slots.reshape(2, DEVS, TILE, TILE), "sp", 1, 1, tiled=True)
        attn_full, lse_full = attend_forward(qkv_full, False)
        o_full = exchange(attn_full)
        qkv_band, attn_full = lax.optimization_barrier((qkv_band, attn_full))
        attn_band, lse_band = attend_forward(qkv_band, True)
        o_band = exchange(attn_band)
        attn_slots = jnp.stack([o_full, o_band])[:, :, None]
        attn_tok = unpack(attn_slots, head_kind, head_k)
        proj_out = dot(attn_tok, w_out).reshape(4, TILE, WIDTH)
        y_out = (x_f + proj_out + b_out.astype(F32)).astype(BF16)
        d_wout = dot(attn_tok, d_y_rows, (((0,), (0,)), ((), ())))

        def halve(part, step):
            bit = lax.rem(lax.div(lax.axis_index("sp"), 2**step), 2)
            axis = 1 if step else 0
            width = part.shape[axis] // 2
            keep = lax.dynamic_slice_in_dim(part, bit * width, width, axis)
            give = lax.dynamic_slice_in_dim(part, width - bit * width, width, axis).astype(BF16)
            take = lax.ppermute(give, "sp", [(i, i ^ 2**step) for i in range(DEVS)])
            return keep + take.astype(F32)

        for step in range(5):
            d_wout = halve(d_wout, step)
        d_qkv_full = attend_backward(qkv_full, d_attn, attn_full, lse_full, False)
        p_full = lax.ppermute(d_qkv_full, "sp", x_swap)
        g_full = exchange(d_qkv_full)
        lse_band, d_qkv_full = lax.optimization_barrier((lse_band, d_qkv_full))
        d_qkv_band = attend_backward(qkv_band, d_attn, attn_band, lse_band, True)
        p_band = lax.ppermute(d_qkv_band, "sp", x_swap)
        g_band = exchange(d_qkv_band)
        d_qkv_slots = jnp.stack([g_full, g_band])

        d_own = regroup(d_qkv_full, d_qkv_band)
        dw_own = dot(d_own, h_all)
        d_part = regroup(p_full, p_band)
        dw_part = dot(d_part, h_all)
        dw_all = jnp.stack([dw_own, dw_part])
        dw_mine = lax.dynamic_slice_in_dim(dw_all, half * ROWS, ROWS, 2)
        dw_other = lax.dynamic_slice_in_dim(dw_all, ROWS - half * ROWS, ROWS, 2)
        dw_other = lax.ppermute(dw_other, "sp", pair_swap)
        dw_sum = (dw_mine + dw_other).astype(BF16).reshape(6, TILE, ROWS).transpose(0, 2, 1)
        shares = jnp.concatenate([dw_sum, d_wout.astype(BF16).reshape(2, ROWS, TILE)])
        shares = lax.all_gather(shares, "sp").reshape(16, 2, 8, ROWS, TILE)
        d_wout = unpack_out(shares)
        d_wqkv = unpack_weights(shares, head_kind, head_k)

        d_qkv_tok = unpack(d_qkv_slots, head_kind, head_k)
        d_bqkv = jnp.sum(d_qkv_tok, axis=0, dtype=F32)
        d_h = dot(d_qkv_tok, w_qkv, NT).astype(BF16).astype(F32).reshape(4, TILE, WIDTH)
        d_x_ln, d_gamma, d_beta = ln_pull(d_h)
        d_x = (d_y.astype(F32) + d_x_ln).astype(BF16)
        d_bout = jnp.sum(d_y_rows, axis=0, dtype=F32)
        d_gamma, d_beta, d_bqkv, d_bout = lax.psum((d_gamma, d_beta, d_bqkv, d_bout), "sp")
        return y_out, d_x, d_gamma, d_beta, d_wqkv, d_bqkv, d_wout, d_bout

    return jax.shard_map(layer, mesh=mesh, in_specs=(tok_spec, tok_spec, P(), P(), P(), P(), P(), P(), P()), out_specs=(tok_spec, tok_spec, P(), P(), P(), P(), P(), P()), check_vma=False)
```

```python
import math
import jax
import jax.numpy as jnp
from jax import lax
from jax.experimental import pallas as pl
from jax.experimental.pallas import tpu as pltpu
from jax.sharding import PartitionSpec as P

LN_EPS = 1e-5
NEG_BIG = -1e30
F32 = jnp.float32
BF16 = jnp.bfloat16
NT = (((1,), (1,)), ((), ()))
NN = (((1,), (0,)), ((), ()))
TILE = 128
WIDTH = 2048
DIM = 64
DEVS = 32
ROWS = 512
BAND = 1024
SEQ = 4096
BQ = 256
BK = 512
LOG2E = 1.4426950408889634


def dot(a, b, dims=NN):
    return lax.dot_general(a, b, dims, preferred_element_type=F32)


def params():
    return pltpu.CompilerParams(vmem_limit_bytes=56 * 2**20)


def low_lanes(shape):
    return lax.broadcasted_iota(jnp.int32, shape, len(shape) - 1) < DIM


def layer_norm(x_rows, gamma_f, beta_f):
    row_mean = jnp.mean(x_rows, axis=-1, keepdims=True)
    centred = x_rows - row_mean
    row_var = jnp.mean(centred * centred, axis=-1, keepdims=True)
    return centred * lax.rsqrt(row_var + LN_EPS) * gamma_f + beta_f


def project_kernel(kind_ref, k_ref, x_ref, w_ref, b_ref, out_ref, buf, sem, *, dims, steps):
    step = pl.program_id(0)
    side = lax.rem(step, 2)

    def copies(at):
        slot = lax.rem(at, 2)
        for i in range(8):
            n = lax.rem(at, 4) * 8 + i
            for half in range(2):
                yield pltpu.make_async_copy(
                    buf.at[slot, i, half],
                    out_ref.at[kind_ref[n], 2 * k_ref[n] + half, lax.div(at, 4)],
                    sem.at[slot],
                )

    @pl.when(step >= 2)
    def _():
        for copy in copies(step - 2):
            copy.wait()

    low = low_lanes((TILE, TILE))
    for pair in range(4):
        cols = slice(pair * TILE, pair * TILE + TILE)
        w_part = w_ref[:, cols] if dims == NN else w_ref[cols, :]
        acc = dot(x_ref[...], w_part, dims) + b_ref[:, cols]
        for half in range(2):
            r0 = acc[half * 256 : half * 256 + TILE]
            r1 = acc[half * 256 + TILE : half * 256 + 256]
            buf[side, 2 * pair, half] = jnp.where(low, r0, pltpu.roll(r1, DIM, 1)).astype(BF16)
            buf[side, 2 * pair + 1, half] = jnp.where(low, pltpu.roll(r0, DIM, 1), r1).astype(BF16)
    for copy in copies(step):
        copy.start()

    @pl.when(step == steps - 1)
    def _():
        for copy in copies(step - 1):
            copy.wait()
        for copy in copies(step):
            copy.wait()


def project(x, w, bias, head_kind, head_k, transposed):
    cols = w.shape[0] if transposed else w.shape[1]
    steps = cols // ROWS
    if transposed:
        w_spec = pl.BlockSpec((ROWS, WIDTH), lambda c, *_: (c, 0))
    else:
        w_spec = pl.BlockSpec((WIDTH, ROWS), lambda c, *_: (0, c))
    body = lambda *refs: project_kernel(*refs, dims=NT if transposed else NN, steps=steps)
    return pl.pallas_call(
        body,
        out_shape=jax.ShapeDtypeStruct((2, DEVS, steps // 4, TILE, TILE), BF16),
        grid_spec=pltpu.PrefetchScalarGridSpec(
            num_scalar_prefetch=2,
            grid=(steps,),
            in_specs=[
                pl.BlockSpec((ROWS, WIDTH), lambda c, *_: (0, 0)),
                w_spec,
                pl.BlockSpec((1, ROWS), lambda c, *_: (0, c)),
            ],
            out_specs=pl.BlockSpec(memory_space=pl.ANY),
            scratch_shapes=[pltpu.VMEM((2, 8, 2, TILE, TILE), BF16), pltpu.SemaphoreType.DMA((2,))],
        ),
        compiler_params=params(),
        cost_estimate=pl.CostEstimate(flops=2 * ROWS * WIDTH * cols, bytes_accessed=WIDTH * cols * 2, transcendentals=0),
        name="project",
    )(head_kind, head_k, x, w, bias)


def unpack_kernel(kind_ref, k_ref, *refs):
    out_ref = refs[8]
    low = low_lanes((TILE, TILE))
    for pair in range(4):
        for half in range(2):
            a = refs[2 * pair][half].astype(F32)
            b = refs[2 * pair + 1][half].astype(F32)
            cols = slice(pair * TILE, pair * TILE + TILE)
            out_ref[half * 256 : half * 256 + TILE, cols] = jnp.where(low, a, pltpu.roll(b, DIM, 1)).astype(BF16)
            out_ref[half * 256 + TILE : half * 256 + 256, cols] = jnp.where(low, pltpu.roll(a, DIM, 1), b).astype(BF16)


def unpack(slots, head_kind, head_k):
    reps = slots.shape[2]
    slots = slots.reshape(2, 16, 2, reps, TILE, TILE)

    def spec(i):
        def index(c, kind_ref, k_ref):
            n = lax.rem(c, 4) * 8 + i
            return kind_ref[n], k_ref[n], 0, lax.div(c, 4), 0, 0

        return pl.BlockSpec((None, None, 2, None, TILE, TILE), index)

    return pl.pallas_call(
        unpack_kernel,
        out_shape=jax.ShapeDtypeStruct((ROWS, reps * WIDTH), BF16),
        grid_spec=pltpu.PrefetchScalarGridSpec(
            num_scalar_prefetch=2,
            grid=(4 * reps,),
            in_specs=[spec(i) for i in range(8)],
            out_specs=pl.BlockSpec((ROWS, ROWS), lambda c, *_: (0, c)),
        ),
        compiler_params=params(),
        cost_estimate=pl.CostEstimate(flops=reps * 2 * 10**9, bytes_accessed=reps * 2**22, transcendentals=0),
        name="unpack",
    )(head_kind, head_k, *([slots] * 8))


def unpack_weights_kernel(kind_ref, k_ref, *refs):
    out_ref = refs[8]
    group = pl.program_id(2)
    low = low_lanes((ROWS, TILE))
    for pair in range(4):
        keep_a = kind_ref[group * 8 + 2 * pair] == 0
        keep_b = kind_ref[group * 8 + 2 * pair + 1] == 1

        def rows_step(r, carry, pair=pair, keep_a=keep_a, keep_b=keep_b):
            a = refs[2 * pair][r].astype(F32)
            b = refs[2 * pair + 1][r].astype(F32)
            a = jnp.where(keep_a, a, pltpu.roll(a, DIM, 1))
            b = jnp.where(keep_b, b, pltpu.roll(b, DIM, 1))
            out_ref[r, :, pair * TILE : pair * TILE + TILE] = jnp.where(low, a, b)
            return carry

        lax.fori_loop(0, 2, rows_step, 0)


def unpack_weights(gathered, head_kind, head_k):
    def spec(i):
        def index(fx, t, g, kind_ref, k_ref):
            k = k_ref[g * 8 + i]
            other = lax.rem(k + fx, 2)
            return lax.div(k, 2) * 2 + fx, 0, other * 3 + t, 0, 0

        return pl.BlockSpec((None, 2, None, ROWS, TILE), index)

    return pl.pallas_call(
        unpack_weights_kernel,
        out_shape=jax.ShapeDtypeStruct((4, ROWS, 3 * WIDTH), F32),
        grid_spec=pltpu.PrefetchScalarGridSpec(
            num_scalar_prefetch=2,
            grid=(2, 3, 4),
            in_specs=[spec(i) for i in range(8)],
            out_specs=pl.BlockSpec((2, ROWS, ROWS), lambda fx, t, g, *_: (fx, 0, t * 4 + g)),
        ),
        compiler_params=params(),
        cost_estimate=pl.CostEstimate(flops=20 * 10**9, bytes_accessed=100 * 2**20, transcendentals=0),
        name="unpack_weights",
    )(head_kind, head_k, *([gathered] * 8)).reshape(WIDTH, 3 * WIDTH)


def unpack_out(gathered):
    def index(c):
        k = lax.rem(c, 2) * 8 + lax.rem(lax.div(c, 2), 2) * 4 + lax.div(c, 8) * 2 + lax.rem(lax.div(c, 4), 2)
        return k, 0, 0, 0

    def body(in_ref, out_ref):
        out_ref[...] = in_ref[...].astype(F32)

    return pl.pallas_call(
        body,
        out_shape=jax.ShapeDtypeStruct((2, BAND, WIDTH), F32),
        grid=(16,),
        in_specs=[pl.BlockSpec((None, 2, BAND, TILE), index)],
        out_specs=pl.BlockSpec((2, BAND, TILE), lambda c: (0, 0, c)),
        compiler_params=params(),
        cost_estimate=pl.CostEstimate(flops=5 * 10**9, bytes_accessed=24 * 2**20, transcendentals=0),
        name="unpack_out",
    )(gathered).reshape(WIDTH, WIDTH)


def regroup_kernel(f_ref, b_ref, out_ref):
    low = low_lanes((TILE, TILE))
    for r in range(4):
        for t in range(3):
            f = f_ref[r, t].astype(F32)
            b = b_ref[r, t].astype(F32)
            rows = slice(t * TILE, t * TILE + TILE)
            even = jnp.where(low, f, pltpu.roll(b, DIM, 1))
            odd = jnp.where(low, pltpu.roll(f, DIM, 1), b)
            out_ref[rows, r * 256 : r * 256 + TILE] = jnp.transpose(even).astype(BF16)
            out_ref[rows, r * 256 + TILE : r * 256 + 256] = jnp.transpose(odd).astype(BF16)


def regroup(f_slots, b_slots):
    spec = pl.BlockSpec((4, 3, TILE, TILE), lambda r: (r, 0, 0, 0))
    return pl.pallas_call(
        regroup_kernel,
        out_shape=jax.ShapeDtypeStruct((384, 8192), BF16),
        grid=(8,),
        in_specs=[spec, spec],
        out_specs=pl.BlockSpec((384, BAND), lambda r: (0, r)),
        compiler_params=params(),
        cost_estimate=pl.CostEstimate(flops=5 * 10**9, bytes_accessed=12 * 2**20, transcendentals=0),
        name="regroup",
    )(f_slots, b_slots)


def split_pair(rows):
    low = low_lanes(rows.shape)
    zero = jnp.zeros_like(rows)
    return jnp.concatenate([jnp.where(low, rows, zero), jnp.where(low, zero, rows)], axis=0)


def load_rows(ref, index, blocks):
    return ref[pl.ds(index * blocks, blocks)].reshape(blocks * TILE, TILE)


def transpose_into(src_ref, dst):
    def step(r, carry):
        cols = pl.ds(pl.multiple_of(r * TILE, TILE), TILE)
        dst[:, cols] = jnp.transpose(src_ref[r].astype(F32)).astype(BF16)
        return carry

    lax.fori_loop(0, DEVS, step, 0)


def allowed_mask(i, j, banded):
    shape = (BK, 2 * BQ)
    diff = lax.broadcasted_iota(jnp.int32, shape, 0) - (lax.broadcasted_iota(jnp.int32, shape, 1) & (BQ - 1))
    off = i * BQ - j * BK
    keep = diff <= off
    if banded:
        keep = keep & (diff > off - BAND)
    return keep


def forward_kernel(q_ref, k_ref, v_ref, o_ref, lse_ref, v_t, *, banded, scale2):
    transpose_into(v_ref, v_t)

    def q_block(i, carry):
        q_pair = split_pair(load_rows(q_ref, i, 2))

        def scores(j, masked):
            s_t = dot(load_rows(k_ref, j, 4), q_pair, NT)
            return jnp.where(allowed_mask(i, j, banded), s_t, NEG_BIG) if masked else s_t

        def weighted(j, p_t):
            cols = pl.ds(pl.multiple_of(j * BK, BK), BK)
            p_t = p_t.astype(BF16)
            return jnp.concatenate(
                [dot(v_t[0:DIM, cols], p_t[:, 0:BQ]), dot(v_t[DIM:TILE, cols], p_t[:, BQ : 2 * BQ])], axis=1
            )

        last = lax.div(i, 2)
        s_t = scores(last, True)
        m = jnp.max(s_t, axis=0, keepdims=True)
        p_t = jnp.exp2((s_t - m) * scale2)
        state = m, jnp.sum(p_t, axis=0, keepdims=True), weighted(last, p_t)

        def k_block(j, state, masked):
            m, l, acc = state
            s_t = scores(j, masked)
            m_new = jnp.maximum(m, jnp.max(s_t, axis=0, keepdims=True))
            p_t = jnp.exp2((s_t - m_new) * scale2)
            fade = jnp.exp2((m - m_new) * scale2)
            return m_new, l * fade + jnp.sum(p_t, axis=0, keepdims=True), acc * fade + weighted(j, p_t)

        if banded:
            near = jnp.maximum(last - 1, 0)
            state = lax.fori_loop(near, last, lambda j, c: k_block(j, c, False), state)
            state = lax.fori_loop(jnp.maximum(last - 2, 0), near, lambda j, c: k_block(j, c, True), state)
        else:
            state = lax.fori_loop(0, last, lambda j, c: k_block(j, c, False), state)
        m, l, acc = state
        out = acc / l
        out = jnp.transpose(jnp.concatenate([out[:, 0:BQ], out[:, BQ : 2 * BQ]], axis=0))
        o_ref[pl.ds(i * 2, 2)] = out.astype(BF16).reshape(2, TILE, TILE)
        lse_ref[pl.ds(i, 1), :] = m * scale2 + jnp.log2(l)
        return carry

    lax.fori_loop(0, SEQ // BQ, q_block, 0)


def attend_forward(qkv, banded):
    scale2 = LOG2E / math.sqrt(DIM)
    whole = lambda t: pl.BlockSpec((DEVS, None, TILE, TILE), lambda g: (0, t, 0, 0))
    tiles = 42 if banded else 72
    return pl.pallas_call(
        lambda *refs: forward_kernel(*refs, banded=banded, scale2=scale2),
        out_shape=(jax.ShapeDtypeStruct((DEVS, TILE, TILE), BF16), jax.ShapeDtypeStruct((16, 2 * BQ), F32)),
        grid=(1,),
        in_specs=[whole(0), whole(1), whole(2)],
        out_specs=(
            pl.BlockSpec((DEVS, TILE, TILE), lambda g: (0, 0, 0)),
            pl.BlockSpec((16, 2 * BQ), lambda g: (0, 0)),
        ),
        scratch_shapes=[pltpu.VMEM((TILE, SEQ), BF16)],
        compiler_params=params(),
        cost_estimate=pl.CostEstimate(flops=tiles * 5 * 10**8, bytes_accessed=2**22, transcendentals=tiles * 2**18),
        name="forward_band" if banded else "forward_full",
    )(qkv, qkv, qkv)


def backward_kernel(q_ref, k_ref, v_ref, do_ref, o_ref, lse_ref, out_ref, k_t, dq_t, delta, dk_acc, dv_acc, *, banded, scale, scale2):
    transpose_into(k_ref, k_t)

    def prepare(i, carry):
        prod = jnp.transpose(load_rows(do_ref, i, 2).astype(F32) * load_rows(o_ref, i, 2).astype(F32))
        delta[pl.ds(i, 1), :] = jnp.concatenate(
            [jnp.sum(prod[0:DIM], axis=0, keepdims=True), jnp.sum(prod[DIM:TILE], axis=0, keepdims=True)], axis=1
        )
        dq_t[i] = jnp.zeros((TILE, BQ), F32)
        return carry

    lax.fori_loop(0, SEQ // BQ, prepare, 0)

    def k_block(j, carry):
        k_rows = load_rows(k_ref, j, 4)
        v_rows = load_rows(v_ref, j, 4)
        cols = pl.ds(pl.multiple_of(j * BK, BK), BK)
        dk_acc[...] = jnp.zeros_like(dk_acc)
        dv_acc[...] = jnp.zeros_like(dv_acc)

        def q_block(i, carry, masked):
            q_pair = split_pair(load_rows(q_ref, i, 2))
            do_pair = split_pair(load_rows(do_ref, i, 2))
            p_t = jnp.exp2(dot(k_rows, q_pair, NT) * scale2 - lse_ref[pl.ds(i, 1), :])
            if masked:
                p_t = jnp.where(allowed_mask(i, j, banded), p_t, 0.0)
            dp_t = dot(v_rows, do_pair, NT).astype(BF16).astype(F32)
            ds_t = (p_t * (dp_t - delta[pl.ds(i, 1), :]) * scale).astype(BF16)
            dv_acc[...] += dot(p_t.astype(BF16), do_pair)
            dk_acc[...] += dot(ds_t, q_pair)
            dq_t[i, 0:DIM, :] += dot(k_t[0:DIM, cols], ds_t[:, 0:BQ])
            dq_t[i, DIM:TILE, :] += dot(k_t[DIM:TILE, cols], ds_t[:, BQ : 2 * BQ])
            return carry

        first = 2 * j
        lax.fori_loop(first, first + 2, lambda i, c: q_block(i, c, True), 0)
        if banded:
            edge = jnp.minimum(first + 4, 16)
            lax.fori_loop(first + 2, edge, lambda i, c: q_block(i, c, False), 0)
            lax.fori_loop(edge, jnp.minimum(first + 6, 16), lambda i, c: q_block(i, c, True), 0)
        else:
            lax.fori_loop(first + 2, 16, lambda i, c: q_block(i, c, False), 0)
        out_ref[pl.ds(j * 4, 4), 1] = dk_acc[...].astype(BF16).reshape(4, TILE, TILE)
        out_ref[pl.ds(j * 4, 4), 2] = dv_acc[...].astype(BF16).reshape(4, TILE, TILE)
        return carry

    lax.fori_loop(0, SEQ // BK, k_block, 0)

    def finish(i, carry):
        out_ref[pl.ds(i * 2, 2), 0] = jnp.transpose(dq_t[i]).astype(BF16).reshape(2, TILE, TILE)
        return carry

    lax.fori_loop(0, SEQ // BQ, finish, 0)


def attend_backward(qkv, d_out, out, lse, banded):
    scale = 1.0 / math.sqrt(DIM)
    whole = lambda t: pl.BlockSpec((DEVS, None, TILE, TILE), lambda g: (0, t, 0, 0))
    flat = pl.BlockSpec((DEVS, TILE, TILE), lambda g: (0, 0, 0))
    of_kind = pl.BlockSpec((None, DEVS, TILE, TILE), lambda g: (1 if banded else 0, 0, 0, 0))
    tiles = 42 if banded else 72
    return pl.pallas_call(
        lambda *refs: backward_kernel(*refs, banded=banded, scale=scale, scale2=scale * LOG2E),
        out_shape=jax.ShapeDtypeStruct((DEVS, 3, TILE, TILE), BF16),
        grid=(1,),
        in_specs=[whole(0), whole(1), whole(2), of_kind, flat, pl.BlockSpec((16, 2 * BQ), lambda g: (0, 0))],
        out_specs=pl.BlockSpec((DEVS, 3, TILE, TILE), lambda g: (0, 0, 0, 0)),
        scratch_shapes=[
            pltpu.VMEM((TILE, SEQ), BF16),
            pltpu.VMEM((16, TILE, BQ), F32),
            pltpu.VMEM((16, 2 * BQ), F32),
            pltpu.VMEM((BK, TILE), F32),
            pltpu.VMEM((BK, TILE), F32),
        ],
        compiler_params=params(),
        cost_estimate=pl.CostEstimate(flops=tiles * 10**9, bytes_accessed=2**23, transcendentals=tiles * 2**18),
        name="backward_band" if banded else "backward_full",
    )(qkv, qkv, qkv, d_out, out, lse)


def exchange(slots):
    return lax.all_to_all(slots, "sp", 0, 0, tiled=True)


def solution(mesh):
    tok_spec = P(None, "sp", None)
    pair_swap = [(i, i ^ 1) for i in range(DEVS)]
    x_swap = [(i, i ^ 2) for i in range(DEVS)]
    same_xc = [list(range(c, DEVS, 4)) for c in range(4)]

    def layer(x, d_y, ln_gamma, ln_beta, w_qkv, b_qkv, w_out, b_out, head_kind):
        half = lax.rem(lax.axis_index("sp"), 2)
        x_bit = lax.rem(lax.div(lax.axis_index("sp"), 2), 2)
        head = jnp.arange(DEVS)
        banded_before = jnp.sum(jnp.where(head[None, :] < head[:, None], head_kind[None, :], 0), axis=1)
        head_k = jnp.where(head_kind == 1, banded_before, head - banded_before).astype(jnp.int32)

        x_f = x.astype(F32)
        h_f, ln_pull = jax.vjp(layer_norm, x_f, ln_gamma.astype(F32), ln_beta.astype(F32))
        h_norm = h_f.astype(BF16)
        d_y_rows = d_y.reshape(ROWS, WIDTH)

        def trade(array, bit, width, axis, flip):
            keep = lax.dynamic_slice_in_dim(array, bit * width, width, axis)
            take = lax.ppermute(lax.dynamic_slice_in_dim(array, width - bit * width, width, axis), "sp", flip)
            return jnp.where(bit == 0, jnp.stack([keep, take]), jnp.stack([take, keep]))

        h_part = trade(h_norm, half, 2, 0, pair_swap)
        h_part = trade(h_part, x_bit, BAND, 3, x_swap)
        qkv_slots = project(h_norm.reshape(ROWS, WIDTH), w_qkv, b_qkv.astype(F32).reshape(1, 3 * WIDTH), head_kind, head_k, False)
        d_attn_slots = project(d_y_rows, w_out, jnp.zeros((1, WIDTH), F32), head_kind, head_k, True)
        qkv_full = exchange(qkv_slots[0])
        qkv_band = exchange(qkv_slots[1])
        qkv_full, d_attn_slots = lax.optimization_barrier((qkv_full, d_attn_slots))
        d_attn = lax.all_to_all(d_attn_slots.reshape(2, DEVS, TILE, TILE), "sp", 1, 1, tiled=True)
        attn_full, lse_full = attend_forward(qkv_full, False)
        o_full = exchange(attn_full)
        qkv_band, attn_full, h_part = lax.optimization_barrier((qkv_band, attn_full, h_part))
        h_all = lax.all_gather(h_part, "sp", axis_index_groups=same_xc).reshape(2 * SEQ, BAND)
        attn_band, lse_band = attend_forward(qkv_band, True)
        o_band = exchange(attn_band)
        attn_slots = jnp.stack([o_full, o_band])[:, :, None]
        attn_tok = unpack(attn_slots, head_kind, head_k)
        proj_out = dot(attn_tok, w_out).reshape(4, TILE, WIDTH)
        y_out = (x_f + proj_out + b_out.astype(F32)).astype(BF16)
        d_wout = dot(attn_tok, d_y_rows, (((0,), (0,)), ((), ())))

        def halve(part, step):
            bit = lax.rem(lax.div(lax.axis_index("sp"), 2**step), 2)
            axis = 1 if step else 0
            width = part.shape[axis] // 2
            keep = lax.dynamic_slice_in_dim(part, bit * width, width, axis)
            give = lax.dynamic_slice_in_dim(part, width - bit * width, width, axis).astype(BF16)
            take = lax.ppermute(give, "sp", [(i, i ^ 2**step) for i in range(DEVS)])
            return keep + take.astype(F32)

        for step in (0, 2, 1, 3, 4):
            d_wout = halve(d_wout, step)
        d_qkv_band = attend_backward(qkv_band, d_attn, attn_band, lse_band, True)
        p_band = lax.ppermute(d_qkv_band, "sp", x_swap)
        g_band = exchange(d_qkv_band)
        lse_full, d_qkv_band = lax.optimization_barrier((lse_full, d_qkv_band))
        d_qkv_full = attend_backward(qkv_full, d_attn, attn_full, lse_full, False)
        p_full = lax.ppermute(d_qkv_full, "sp", x_swap)
        g_full = exchange(d_qkv_full)
        d_qkv_slots = jnp.stack([g_full, g_band])

        d_own = regroup(d_qkv_full, d_qkv_band)
        dw_own = dot(d_own, h_all)
        d_part = regroup(p_full, p_band)
        dw_part = dot(d_part, h_all)
        dw_all = jnp.stack([dw_own, dw_part])
        dw_mine = lax.dynamic_slice_in_dim(dw_all, half * ROWS, ROWS, 2)
        dw_other = lax.dynamic_slice_in_dim(dw_all, ROWS - half * ROWS, ROWS, 2)
        dw_other = lax.ppermute(dw_other, "sp", pair_swap)
        dw_sum = (dw_mine + dw_other).astype(BF16).reshape(6, TILE, ROWS).transpose(0, 2, 1)
        d_wout = lax.all_gather(d_wout.astype(BF16), "sp").reshape(16, 2, BAND, TILE)
        d_wout = unpack_out(d_wout)
        shares = lax.all_gather(dw_sum, "sp").reshape(16, 2, 6, ROWS, TILE)
        d_wqkv = unpack_weights(shares, head_kind, head_k)

        d_qkv_tok = unpack(d_qkv_slots, head_kind, head_k)
        d_bqkv = jnp.sum(d_qkv_tok, axis=0, dtype=F32)
        d_h = dot(d_qkv_tok, w_qkv, NT).astype(BF16).astype(F32).reshape(4, TILE, WIDTH)
        d_x_ln, d_gamma, d_beta = ln_pull(d_h)
        d_x = (d_y.astype(F32) + d_x_ln).astype(BF16)
        d_bout = jnp.sum(d_y_rows, axis=0, dtype=F32)
        d_gamma, d_beta, d_bqkv, d_bout = lax.psum((d_gamma, d_beta, d_bqkv, d_bout), "sp")
        return y_out, d_x, d_gamma, d_beta, d_wqkv, d_bqkv, d_wout, d_bout

    return jax.shard_map(layer, mesh=mesh, in_specs=(tok_spec, tok_spec, P(), P(), P(), P(), P(), P(), P()), out_specs=(tok_spec, tok_spec, P(), P(), P(), P(), P(), P()), check_vma=False)
```
